512 devices in a mesh: graph: 32 (over z, x), dp: 16 (over y, core).
Axes of the slice: x: 4, y: 8, z: 8, core: 2. Of those that a mesh axis runs over, the one named last changes fastest.
Arguments:
- node_state: bfloat16 [16, 16384, 512], P('dp', 'graph'), may hold values from -6 to 6
- edge_state: bfloat16 [16, 65536, 512], P('dp', 'graph'), may hold values from -6 to 6
- senders: int32 [16, 65536], P('dp', 'graph'), may hold values from 0 to 767
- receivers: int32 [16, 65536], P('dp', 'graph'), may hold values from 0 to 511
- send_index: int32 [16, 32, 256], P('dp', 'graph'), may hold values from 0 to 511
- cotangent: bfloat16 [16, 16384, 512], P('dp', 'graph'), may hold values from -0.046875 to 0.046875
- w_edge: bfloat16 [1536, 512], replicated, may hold values from -0.15625 to 0.15625
- w_node: bfloat16 [1024, 512], replicated, may hold values from -0.1875 to 0.1875
- error_memory: float32 [16, 1024, 512], P('dp', 'graph'), may hold values from -6 to 6
- warm_q: float32 [512, 64], replicated, may hold values from -6 to 6
Outputs:
- new_nodes: bfloat16 [16, 16384, 512], P('dp', 'graph')
- update: float32 [1024, 512], P('graph')
- new_error: float32 [16, 1024, 512], P('dp', 'graph')
- new_q: float32 [512, 64], replicated
The draws below stay inside these ranges and needn't reach their ends.
All inputs are finite; a program needn't handle non-finite values.
Results may differ from the reference program's by a relative error of at most 0.0066.
Values may be sent and summed in bfloat16 or wider, within the bound.
A program may use at most 64 MiB of HBM per device.

```python
import jax
import jax.numpy as jnp
from jax import lax

D = 512
RANK = 64
NODE_DEV = 512
PEER = 8
EDGE_DEV = 2048
NODES = 16384
EDGES = 65536
N_GRAPH = 32
N_DP = 16


def touch_ends(result, rng, least, largest):
    longest = result.shape.index(max(result.shape))
    spots = []
    for shift in (0, 1):
        where = [jax.random.randint(jax.random.fold_in(rng, axis), (), 0, length) for axis, length in enumerate(result.shape)]
        where[longest] = (where[longest] + shift) % result.shape[longest]
        spots.append(tuple(where))
    return result.at[spots[0]].set(least).at[spots[1]].set(largest)


def level_of(key, extent, cuts, smallest, top_value):
    level = 1.0
    for axis_at, blocks in cuts:
        heights = jax.random.uniform(jax.random.fold_in(jax.random.fold_in(key, 6), axis_at), (blocks,), jnp.float32, smallest / len(cuts), top_value / len(cuts))
        level = level * jnp.repeat(jnp.exp(heights), extent[axis_at] // blocks).reshape((-1,) + (1,) * (len(extent) - 1 - axis_at))
    return level


def gaussian(rng, dims, scale, limit, shards=(), held_as=jnp.bfloat16):
    result = scale * jax.random.normal(rng, dims, jnp.float32)
    if shards:
        result = result * level_of(rng, dims, shards, -0.22, 0.18)
    return jnp.clip(result, -limit, limit).astype(held_as)


def setup_inputs(seed: int = 0) -> dict:
    keys = jax.random.split(jax.random.key(seed), 11)
    node_state = gaussian(keys[0], (N_DP, NODES, D), 1.0, 6.0, ((0, 16), (1, 32)))
    edge_state = gaussian(keys[1], (N_DP, EDGES, D), 1.0, 6.0, ((0, 16), (1, 32)))
    senders = touch_ends(jax.random.randint(keys[2], (N_DP, EDGES), 0, NODE_DEV + N_GRAPH * PEER), jax.random.fold_in(keys[2], 1), 0, (NODE_DEV + N_GRAPH * PEER) - 1).astype(jnp.int32)
    receivers = touch_ends(jax.random.randint(keys[3], (N_DP, EDGES), 0, NODE_DEV), jax.random.fold_in(keys[3], 1), 0, NODE_DEV - 1).astype(jnp.int32)
    send_index = touch_ends(jax.random.randint(keys[4], (N_DP, N_GRAPH, N_GRAPH * PEER), 0, NODE_DEV), jax.random.fold_in(keys[4], 1), 0, NODE_DEV - 1).astype(jnp.int32)
    cotangent = gaussian(keys[5], (N_DP, NODES, D), (1.0 / (N_GRAPH * NODE_DEV) ** 0.5), 0.046875, ((0, 16), (1, 32)))
    w_edge = gaussian(keys[6], (3 * D, D), (3 * D) ** -0.5, 0.15625)
    w_node = gaussian(keys[7], (2 * D, D), (2 * D) ** -0.5, 0.1875)
    error_memory = gaussian(keys[8], (N_DP, 2 * D, D), 1.0, 6.0, ((0, 16), (1, 32)), jnp.float32)
    warm_q = gaussian(keys[9], (D, RANK), 1.0, 6.0, (), jnp.float32)
    return dict(node_state=node_state, edge_state=edge_state, senders=senders, receivers=receivers, send_index=send_index, cotangent=cotangent, w_edge=w_edge, w_node=w_node, error_memory=error_memory, warm_q=warm_q)


def silu_slope(pre_act):
    sigmoid_v = jax.nn.sigmoid(pre_act)
    return sigmoid_v * (1.0 + pre_act * (1.0 - sigmoid_v))

def one_group(inputs):
    node_state, edge_state, senders, receivers, send_index, cotangent, w_edge, w_node = inputs
    offsets = (jnp.arange(N_GRAPH, dtype=jnp.int32) * NODE_DEV)[:, None]

    def partition(grad_total, index):
        node_block = lax.dynamic_slice_in_dim(node_state, (index * NODE_DEV).astype(jnp.int32), NODE_DEV, 0)
        cot_block = lax.dynamic_slice_in_dim(cotangent, (index * NODE_DEV).astype(jnp.int32), NODE_DEV, 0)
        edge_block = lax.dynamic_slice_in_dim(edge_state, (index * EDGE_DEV).astype(jnp.int32), EDGE_DEV, 0)
        send_block = lax.dynamic_slice_in_dim(senders, (index * EDGE_DEV).astype(jnp.int32), EDGE_DEV, 0)
        recv_block = lax.dynamic_slice_in_dim(receivers, (index * EDGE_DEV).astype(jnp.int32), EDGE_DEV, 0)
        chosen_rows = lax.dynamic_slice_in_dim(send_index, (index * PEER).astype(jnp.int32), PEER, 1)
        global_rows = (chosen_rows + offsets).reshape(-1)
        halo = node_state[global_rows]
        lookup = jnp.concatenate([node_block, halo], axis=0)
        sender_rows = lookup[send_block]
        receiver_rows = node_block[recv_block]
        joined = jnp.concatenate([edge_block, sender_rows, receiver_rows], axis=1)
        edge_pre = jnp.dot(joined.astype(jnp.float32), w_edge.astype(jnp.float32), preferred_element_type=jnp.float32)
        edge_new = (edge_block.astype(jnp.float32) + jax.nn.silu(edge_pre)).astype(jnp.bfloat16)
        aggregate = jax.ops.segment_sum(edge_new.astype(jnp.float32), recv_block, num_segments=NODE_DEV).astype(jnp.bfloat16)
        node_input = jnp.concatenate([node_block, aggregate], axis=1)
        node_pre = jnp.dot(node_input.astype(jnp.float32), w_node.astype(jnp.float32), preferred_element_type=jnp.float32)
        new_block = (node_block.astype(jnp.float32) + jax.nn.silu(node_pre)).astype(jnp.bfloat16)
        node_delta = (cot_block.astype(jnp.float32) * silu_slope(node_pre)).astype(jnp.bfloat16)
        grad_part = jnp.dot(node_input.T.astype(jnp.float32), node_delta.astype(jnp.float32), preferred_element_type=jnp.float32)
        return (grad_total + grad_part, new_block)
    start = jnp.zeros((2 * D, D), jnp.float32)
    grad_total, blocks = lax.scan(partition, start, jnp.arange(N_GRAPH, dtype=jnp.int32))
    return (blocks.reshape(NODES, D), grad_total)

def reference(node_state, edge_state, senders, receivers, send_index, cotangent, w_edge, w_node, error_memory, warm_q):

    def run_group(inputs):
        return one_group(inputs + (w_edge, w_node))
    new_nodes, gradient = lax.map(run_group, (node_state, edge_state, senders, receivers, send_index, cotangent))
    highest = lax.Precision.HIGHEST
    matrix = gradient + error_memory
    left = jnp.einsum('gij,jr->ir', matrix, warm_q, precision=highest)
    gram = jnp.dot(left.T, left, precision=highest)
    chol = jnp.linalg.cholesky(gram)
    ortho = lax.linalg.triangular_solve(chol, left, left_side=False, lower=True, transpose_a=True)
    new_q = jnp.einsum('gij,ir->jr', matrix, ortho, precision=highest) / N_DP
    update = jnp.dot(ortho, new_q.T, precision=highest)
    new_error = matrix - update[None]
    return (new_nodes, update, new_error, new_q)
```

```python
import functools

import jax
import jax.numpy as jnp
from jax import lax
from jax.experimental import pallas as pl
from jax.experimental.pallas import tpu as pltpu
from jax.sharding import Mesh
from jax.sharding import PartitionSpec as P

AXES = ("graph_0", "graph_1", "dp_0", "dp_1")
GRAPH = AXES[:2]
DP = AXES[2:]
MESH = pl.DeviceIdType.MESH
BF = jnp.bfloat16
F32 = jnp.float32
HIGH = lax.Precision.HIGHEST
LANE = 128


def mm(a, b, dims=((1,), (0,)), precision=None):
    return lax.dot_general(a, b, (dims, ((), ())), precision=precision, preferred_element_type=F32)


def sigmoid(v):
    return 0.5 + 0.5 * jnp.tanh(0.5 * v)


def column(row):
    eye = lax.broadcasted_iota(jnp.int32, (LANE, LANE), 0) == lax.broadcasted_iota(
        jnp.int32, (LANE, LANE), 1
    )
    return jnp.sum(jnp.where(eye, row, 0.0), axis=1, keepdims=True)


def one_hot(col, width, base=0):
    lanes = lax.broadcasted_iota(jnp.int32, (col.shape[0], width), 1) + base
    return jnp.where(lanes.astype(F32) == col, 1.0, 0.0).astype(BF)


def inverse_factor(gram):
    n = gram.shape[0]
    rows = lax.broadcasted_iota(jnp.int32, (n, 1), 0)
    eye = jnp.where(
        lax.broadcasted_iota(jnp.int32, (n, n), 0) == lax.broadcasted_iota(jnp.int32, (n, n), 1),
        1.0,
        0.0,
    ).astype(F32)
    work = jnp.concatenate([gram, eye], axis=1)
    for k in range(n - 1):
        pivot = work[k : k + 1, :]
        scaled = pivot / pivot[:, k : k + 1]
        work = work - jnp.where(rows > k, work[:, k : k + 1], 0.0) * scaled
    diagonal = jnp.sum(work[:, :n] * eye, axis=1, keepdims=True)
    return work[:, n:] / jnp.sqrt(diagonal)


def kernel(
    sizes,
    node_hbm,
    edge_hbm,
    senders_hbm,
    receivers_hbm,
    send_hbm,
    cot_hbm,
    w_edge_hbm,
    w_node_hbm,
    error_hbm,
    warm_hbm,
    new_nodes_hbm,
    update_ref,
    new_error_ref,
    new_q_ref,
    node,
    edge,
    senders,
    receivers,
    send_index,
    cot,
    w_edge,
    w_node,
    error,
    warm,
    load_sem,
    store_sem,
    halo_out,
    halo_in,
    own_p,
    own_r,
    halo_p,
    pre,
    pick_halo,
    incidence,
    total,
    new_block,
    delta,
    inputs_t,
    grad_a,
    grad_b,
    ax_in,
    ax_sum,
    az_in,
    bz_in,
    b_sum,
    bx_in,
    matrix,
    dp_out,
    dp_in,
    z_out,
    z_in,
    x_out,
    x_in,
    q_out,
    q_in,
    halo_s,
    halo_r,
    ax_s,
    ax_r,
    az_s,
    az_r,
    bz_s,
    bz_r,
    bx_s,
    bx_r,
    dp_s,
    dp_r,
    z_s,
    z_r,
    x_s,
    x_r,
    q_s,
    q_r,
):
    nz, nx, ny, nc, cut, tile = sizes
    ng, nd = nz * nx, ny * nc
    count, width = node.shape
    edges = edge.shape[0]
    tiles = edges // tile
    chunks = tile // LANE
    z, x = lax.axis_index(AXES[0]), lax.axis_index(AXES[1])
    y, c = lax.axis_index(AXES[2]), lax.axis_index(AXES[3])
    part = z * nx + x
    group = y * nc + c

    def on_graph(index):
        return (index // nx, lax.rem(index, nx), y, c)

    def on_dp(index):
        return (z, x, index // nc, lax.rem(index, nc))

    def on_z(index):
        return (index, x, y, c)

    def on_x(index):
        return (z, index, y, c)

    def remote(src, dst, send, recv, device):
        return pltpu.make_async_remote_copy(
            src_ref=src,
            dst_ref=dst,
            send_sem=send,
            recv_sem=recv,
            device_id=device,
            device_id_type=MESH,
        )

    loads = [
        pltpu.make_async_copy(src, dst, load_sem.at[i])
        for i, (src, dst) in enumerate(
            [
                (send_hbm, send_index),
                (node_hbm, node),
                (receivers_hbm, receivers),
                (senders_hbm, senders),
                (w_edge_hbm, w_edge),
                (edge_hbm, edge),
                (w_node_hbm, w_node),
                (cot_hbm, cot),
                (error_hbm, error),
                (warm_hbm, warm),
            ]
        )
    ]
    for load in loads:
        load.start()

    barrier = pltpu.get_barrier_semaphore()

    @pl.loop(1, ng)
    def _(o):
        pl.semaphore_signal(
            barrier, inc=1, device_id=on_graph(lax.rem(part + o, ng)), device_id_type=MESH
        )

    @pl.loop(1, nd)
    def _(o):
        pl.semaphore_signal(
            barrier, inc=1, device_id=on_dp(lax.rem(group + o, nd)), device_id_type=MESH
        )

    loads[0].wait()
    loads[1].wait()
    half = width // 2
    peer = send_index.shape[0] * LANE // ng
    per = LANE // peer
    for i in range(send_index.shape[0]):
        col = column(send_index[i : i + 1, :].astype(F32))
        rows = mm(one_hot(col, count), node[...])
        pair = jnp.concatenate(
            [
                rows[:, :half].reshape(per, peer, half),
                rows[:, half:].reshape(per, peer, half),
            ],
            axis=1,
        )
        halo_out[i * per : (i + 1) * per] = pair.astype(BF)
    halo_in[pl.ds(part, 1)] = halo_out[pl.ds(part, 1)]

    pl.semaphore_wait(barrier, ng - 1 + nd - 1)

    def halo_copy(o):
        to = lax.rem(part + o, ng)
        return remote(
            halo_out.at[to], halo_in.at[part], halo_s.at[o - 1], halo_r.at[o - 1], on_graph(to)
        )

    @pl.loop(1, ng)
    def _(o):
        halo_copy(o).start()

    loads[2].wait()
    loads[3].wait()
    loads[4].wait()
    own_p[...] = mm(node[...], w_edge[width : 2 * width, :]).astype(BF)
    own_r[...] = mm(node[...], w_edge[2 * width :, :]).astype(BF)
    loads[5].wait()

    @pl.loop(0, tiles)
    def _(t):
        at = pl.ds(pl.multiple_of(t * tile, tile), tile)
        from_col = jnp.concatenate(
            [
                column(senders[pl.ds(t * chunks + j, 1), :].astype(F32))
                for j in range(chunks)
            ],
            axis=0,
        )
        to_rows = [receivers[pl.ds(t * chunks + j, 1), :].astype(F32) for j in range(chunks)]
        to_col = jnp.concatenate([column(row) for row in to_rows], axis=0)
        value = mm(edge[at, :], w_edge[:width, :])
        value = value + mm(one_hot(from_col, count), own_p[...])
        value = value + mm(one_hot(to_col, count), own_r[...])
        pre[at, :] = value
        pick_halo[at, :] = one_hot(from_col, halo_p.shape[0], count)
        ids = lax.broadcasted_iota(jnp.int32, (count, LANE), 0).astype(F32)
        for j, row in enumerate(to_rows):
            incidence[t, :, j * LANE : (j + 1) * LANE] = jnp.where(ids == row, 1.0, 0.0).astype(BF)

    inputs_t[:width, :] = node[...].astype(F32).T.astype(BF)

    @pl.loop(1, ng)
    def _(o):
        halo_copy(o).wait()

    flat = halo_in[...].reshape(ng * 2 * peer, half)
    left_half = mm(flat, w_edge[width : width + half, :]).reshape(ng, 2, peer, width)
    right_half = mm(flat, w_edge[width + half : 2 * width, :]).reshape(ng, 2, peer, width)
    halo_p[...] = (left_half[:, 0] + right_half[:, 1]).reshape(ng * peer, width).astype(BF)

    total[...] = jnp.zeros_like(total)

    @pl.loop(0, tiles)
    def _(t):
        at = pl.ds(pl.multiple_of(t * tile, tile), tile)
        value = pre[at, :] + mm(pick_halo[at, :], halo_p[...])
        fresh = (edge[at, :].astype(F32) + value * sigmoid(value)).astype(BF)
        total[...] += mm(incidence[t], fresh)

    loads[6].wait()
    loads[7].wait()
    summed = total[...].astype(BF)
    node_pre = mm(node[...], w_node[:width, :]) + mm(summed, w_node[width:, :])
    gate = sigmoid(node_pre)
    delta[...] = (cot[...].astype(F32) * (gate * (1.0 + node_pre * (1.0 - gate)))).astype(BF)
    new_block[...] = (node[...].astype(F32) + node_pre * gate).astype(BF)
    store = pltpu.make_async_copy(new_block, new_nodes_hbm, store_sem.at[0])
    store.start()
    inputs_t[width:, :] = total[...].T.astype(BF)

    share = 2 * width // ng
    step = min(nz, max(1, 256 // (nx * share)))

    @pl.loop(0, nz // step)
    def _(i):
        lines = step * nx * share
        grad = mm(inputs_t[pl.ds(pl.multiple_of(i * lines, lines), lines), :], delta[...])
        at = pl.ds(i * step, step)
        grad_a[at] = grad[:, :cut].reshape(step, nx, share, cut).astype(BF)
        grad_b[at] = grad[:, cut:].reshape(step, nx, share, width - cut).astype(BF)

    z_order = sorted(range(1, nz), key=lambda o: -min(o, nz - o))
    x_order = sorted(range(1, nx), key=lambda o: -min(o, nx - o))
    turns = z_order + [0]

    def z_at(o):
        return lax.rem(z + o, nz)

    def x_at(o):
        return lax.rem(x + o, nx)

    bz = {
        o: remote(
            grad_b.at[z_at(o)], bz_in.at[o - 1], bz_s.at[o - 1], bz_r.at[o - 1], on_z(z_at(o))
        )
        for o in z_order
    }
    ax = {
        (t, o): remote(
            grad_a.at[z_at(t), x_at(o)],
            ax_in.at[o - 1, t],
            ax_s.at[o - 1, t],
            ax_r.at[o - 1, t],
            on_x(x_at(o)),
        )
        for t in turns
        for o in x_order
    }
    az = {
        o: remote(ax_sum.at[o], az_in.at[o - 1], az_s.at[o - 1], az_r.at[o - 1], on_z(z_at(o)))
        for o in z_order
    }
    bx = {
        o: remote(
            b_sum.at[x_at(o)], bx_in.at[o - 1], bx_s.at[o - 1], bx_r.at[o - 1], on_x(x_at(o))
        )
        for o in x_order
    }
    for copy in bz.values():
        copy.start()
    for copy in ax.values():
        copy.start()
    for t in turns:
        value = grad_a[z_at(t), x].astype(F32)
        for o in x_order:
            ax[t, o].wait_recv()
            value = value + ax_in[o - 1, t].astype(F32)
        if t:
            ax_sum[t] = value.astype(BF)
            az[t].start()
        else:
            own_a = value
    value = grad_b[z].astype(F32)
    for o in z_order:
        bz[o].wait_recv()
        value = value + bz_in[o - 1].astype(F32)
    b_sum[...] = value.astype(BF)
    for copy in bx.values():
        copy.start()
    own_b = b_sum[x].astype(F32)
    for o in x_order:
        bx[o].wait_recv()
        own_b = own_b + bx_in[o - 1].astype(F32)
    for o in z_order:
        az[o].wait_recv()
        own_a = own_a + az_in[o - 1].astype(F32)
    loads[8].wait()
    loads[9].wait()
    matrix[:, :cut] = own_a + error[:, :cut]
    matrix[:, cut:] = own_b + error[:, cut:]

    rank = warm.shape[0]
    pack = LANE // rank
    blocks = width // LANE
    piece = LANE // nd
    local = mm(matrix[...], warm[...], ((1,), (1,)), HIGH)
    packed = jnp.concatenate([local[: share // 2], local[share // 2 :]], axis=1)
    turned = jnp.concatenate(
        [matrix[:, q * LANE : (q + 1) * LANE] for q in range(blocks)], axis=0
    ).T
    dp_out[:, :piece, :] = turned.reshape(nd, piece, LANE)
    dp_out[:, piece:, :] = jnp.broadcast_to(packed[None], (nd, *packed.shape))
    dp_in[pl.ds(group, 1)] = dp_out[pl.ds(group, 1)]

    def dp_copy(o):
        to = lax.rem(group + o, nd)
        return remote(dp_out.at[to], dp_in.at[group], dp_s.at[o - 1], dp_r.at[o - 1], on_dp(to))

    @pl.loop(1, nd)
    def _(o):
        dp_copy(o).start()

    @pl.loop(1, nd)
    def _(o):
        dp_copy(o).wait()

    arrived = jnp.sum(dp_in[...], axis=0)
    columns, packed = arrived[:piece], arrived[piece:]
    left = jnp.concatenate([packed[:, :rank], packed[:, rank:]], axis=0)
    gram = mm(left, left, ((0,), (0,)), HIGH)
    twice = jnp.concatenate([left, left], axis=1)
    spread = jnp.concatenate([twice] * blocks, axis=0)
    owner = lax.broadcasted_iota(jnp.int32, (LANE, LANE), 0) // share
    side = lax.broadcasted_iota(jnp.int32, (LANE, LANE), 1) // rank
    halves = blocks // pack
    for h in range(halves):
        chosen = jnp.where(owner == pack * h + side, spread, 0.0)
        z_out[h * piece : (h + 1) * piece, :] = mm(columns, chosen, precision=HIGH)
    z_out[halves * piece :, :] = jnp.concatenate([gram[: rank // 2], gram[rank // 2 :]], axis=1)

    z_in[pl.ds(z, 1)] = z_out[...][None]
    zs = {
        o: remote(z_out, z_in.at[z], z_s.at[o - 1], z_r.at[o - 1], on_z(z_at(o)))
        for o in z_order
    }
    for copy in zs.values():
        copy.start()
    for copy in zs.values():
        copy.wait()
    x_out[...] = jnp.sum(z_in[...], axis=0)
    x_in[pl.ds(x, 1)] = x_out[...][None]
    xs = {
        o: remote(x_out, x_in.at[x], x_s.at[o - 1], x_r.at[o - 1], on_x(x_at(o)))
        for o in x_order
    }
    for copy in xs.values():
        copy.start()
    for copy in xs.values():
        copy.wait()
    both = jnp.sum(x_in[...], axis=0)

    q_out[...] = both[: halves * piece]
    q_in[pl.ds(group, 1)] = q_out[...][None]

    def q_copy(o):
        to = lax.rem(group + o, nd)
        return remote(q_out, q_in.at[group], q_s.at[o - 1], q_r.at[o - 1], on_dp(to))

    @pl.loop(1, nd)
    def _(o):
        q_copy(o).start()

    packed = both[halves * piece :]
    gram = jnp.concatenate([packed[:, :rank], packed[:, rank:]], axis=0)
    inverse = inverse_factor(gram)
    ortho = mm(left, inverse, ((1,), (1,)), HIGH)

    @pl.loop(1, nd)
    def _(o):
        q_copy(o).wait()

    for h in range(halves):
        right = q_in[:, h * piece : (h + 1) * piece, :].reshape(LANE, LANE)
        for side in range(pack):
            q = h * pack + side
            at = slice(q * LANE, (q + 1) * LANE)
            new_q = mm(inverse, right[:, side * rank : (side + 1) * rank], ((1,), (1,)), HIGH) / nd
            new_q_ref[:, at] = new_q
            update = mm(ortho, new_q, precision=HIGH)
            update_ref[:, at] = update
            new_error_ref[:, at] = matrix[:, at] - update

    for copies in (bz, ax, az, bx):
        for copy in copies.values():
            copy.wait_send()
    store.wait()


def layer(
    sizes,
    node_state,
    edge_state,
    senders,
    receivers,
    send_index,
    cotangent,
    w_edge,
    w_node,
    error_memory,
    warm_q,
):
    nz, nx, ny, nc, cut, tile = sizes
    ng, nd = nz * nx, ny * nc
    count, width = node_state.shape[1:]
    edges = edge_state.shape[1]
    rank = warm_q.shape[1]
    share = 2 * width // ng
    halo = send_index.shape[-1]
    peer = halo // ng
    piece = LANE // nd
    halves = width * rank // LANE // LANE
    hbm = pl.BlockSpec(memory_space=pltpu.MemorySpace.HBM)
    vmem = pl.BlockSpec(memory_space=pltpu.VMEM)
    dma = pltpu.SemaphoreType.DMA
    exchange = halves * piece + rank // 2
    new_block, update, new_error, new_q = pl.pallas_call(
        functools.partial(kernel, sizes),
        out_shape=(
            jax.ShapeDtypeStruct((count, width), BF),
            jax.ShapeDtypeStruct((share, width), F32),
            jax.ShapeDtypeStruct((share, width), F32),
            jax.ShapeDtypeStruct((rank, width), F32),
        ),
        in_specs=[hbm] * 10,
        out_specs=(hbm, vmem, vmem, vmem),
        scratch_shapes=[
            pltpu.VMEM((count, width), BF),
            pltpu.VMEM((edges, width), BF),
            pltpu.VMEM((edges // LANE, LANE), jnp.int32),
            pltpu.VMEM((edges // LANE, LANE), jnp.int32),
            pltpu.VMEM((halo // LANE, LANE), jnp.int32),
            pltpu.VMEM((count, width), BF),
            pltpu.VMEM((3 * width, width), BF),
            pltpu.VMEM((2 * width, width), BF),
            pltpu.VMEM((share, width), F32),
            pltpu.VMEM((rank, width), F32),
            dma((10,)),
            dma((1,)),
            pltpu.VMEM((ng, 2 * peer, width // 2), BF),
            pltpu.VMEM((ng, 2 * peer, width // 2), BF),
            pltpu.VMEM((count, width), BF),
            pltpu.VMEM((count, width), BF),
            pltpu.VMEM((halo, width), BF),
            pltpu.VMEM((edges, width), F32),
            pltpu.VMEM((edges, halo), BF),
            pltpu.VMEM((edges // tile, count, tile), BF),
            pltpu.VMEM((count, width), F32),
            pltpu.VMEM((count, width), BF),
            pltpu.VMEM((count, width), BF),
            pltpu.VMEM((2 * width, count), BF),
            pltpu.VMEM((nz, nx, share, cut), BF),
            pltpu.VMEM((nz, nx, share, width - cut), BF),
            pltpu.VMEM((nx - 1, nz, share, cut), BF),
            pltpu.VMEM((nz, share, cut), BF),
            pltpu.VMEM((nz - 1, share, cut), BF),
            pltpu.VMEM((nz - 1, nx, share, width - cut), BF),
            pltpu.VMEM((nx, share, width - cut), BF),
            pltpu.VMEM((nx - 1, share, width - cut), BF),
            pltpu.VMEM((share, width), F32),
            pltpu.VMEM((nd, piece + share // 2, LANE), F32),
            pltpu.VMEM((nd, piece + share // 2, LANE), F32),
            pltpu.VMEM((exchange, LANE), F32),
            pltpu.VMEM((nz, exchange, LANE), F32),
            pltpu.VMEM((exchange, LANE), F32),
            pltpu.VMEM((nx, exchange, LANE), F32),
            pltpu.VMEM((halves * piece, LANE), F32),
            pltpu.VMEM((nd, halves * piece, LANE), F32),
            dma((ng - 1,)),
            dma((ng - 1,)),
            dma((nx - 1, nz)),
            dma((nx - 1, nz)),
            dma((nz - 1,)),
            dma((nz - 1,)),
            dma((nz - 1,)),
            dma((nz - 1,)),
            dma((nx - 1,)),
            dma((nx - 1,)),
            dma((nd - 1,)),
            dma((nd - 1,)),
            dma((nz - 1,)),
            dma((nz - 1,)),
            dma((nx - 1,)),
            dma((nx - 1,)),
            dma((nd - 1,)),
            dma((nd - 1,)),
        ],
        compiler_params=pltpu.CompilerParams(
            collective_id=0, has_side_effects=True, vmem_limit_bytes=67043328
        ),
    )(
        node_state[0],
        edge_state[0],
        senders.reshape(-1, LANE),
        receivers.reshape(-1, LANE),
        send_index.reshape(-1, LANE),
        cotangent[0],
        w_edge,
        w_node,
        error_memory[0],
        warm_q.T,
    )
    return new_block[None], update, new_error[None], new_q.T


def build(finer, cut, tile):
    placed = (
        P(DP, GRAPH, None),
        P(DP, GRAPH, None),
        P(DP, GRAPH),
        P(DP, GRAPH),
        P(DP, GRAPH, None),
        P(DP, GRAPH, None),
        P(),
        P(),
        P(DP, GRAPH, None),
        P(),
    )
    sizes = (*(finer.shape[a] for a in AXES), cut, tile)
    return jax.shard_map(
        functools.partial(layer, sizes),
        mesh=finer,
        in_specs=placed,
        out_specs=(P(DP, GRAPH, None), P(GRAPH, None), P(DP, GRAPH, None), P()),
        check_vma=False,
    )


def solution(mesh):
    return build(Mesh(mesh.devices.reshape(8, 4, 8, 2), AXES), 384, 512)
```

```python
import functools

import jax
import jax.numpy as jnp
from jax import lax
from jax.experimental import pallas as pl
from jax.experimental.pallas import tpu as pltpu
from jax.sharding import Mesh
from jax.sharding import PartitionSpec as P

AXES = ("graph_0", "graph_1", "dp_0", "dp_1")
GRAPH = AXES[:2]
DP = AXES[2:]
MESH = pl.DeviceIdType.MESH
BF = jnp.bfloat16
F32 = jnp.float32
HIGH = lax.Precision.HIGHEST
LANE = 128


def mm(a, b, dims=((1,), (0,)), precision=None):
    return lax.dot_general(a, b, (dims, ((), ())), precision=precision, preferred_element_type=F32)


def sigmoid(v):
    return 0.5 + 0.5 * jnp.tanh(0.5 * v)


def column(row):
    eye = lax.broadcasted_iota(jnp.int32, (LANE, LANE), 0) == lax.broadcasted_iota(
        jnp.int32, (LANE, LANE), 1
    )
    return jnp.sum(jnp.where(eye, row, 0.0), axis=1, keepdims=True)


def one_hot(col, width, base=0):
    lanes = lax.broadcasted_iota(jnp.int32, (col.shape[0], width), 1) + base
    return jnp.where(lanes.astype(F32) == col, 1.0, 0.0).astype(BF)


def inverse_factor(gram):
    n = gram.shape[0]
    rows = lax.broadcasted_iota(jnp.int32, (n, 1), 0)
    eye = jnp.where(
        lax.broadcasted_iota(jnp.int32, (n, n), 0) == lax.broadcasted_iota(jnp.int32, (n, n), 1),
        1.0,
        0.0,
    ).astype(F32)
    work = jnp.concatenate([gram, eye], axis=1)
    for k in range(n - 1):
        pivot = work[k : k + 1, :]
        scaled = pivot / pivot[:, k : k + 1]
        work = work - jnp.where(rows > k, work[:, k : k + 1], 0.0) * scaled
    diagonal = jnp.sum(work[:, :n] * eye, axis=1, keepdims=True)
    return work[:, n:] / jnp.sqrt(diagonal)


def kernel(
    sizes,
    node_hbm,
    edge_hbm,
    senders_hbm,
    receivers_hbm,
    send_hbm,
    cot_hbm,
    w_edge_hbm,
    w_node_hbm,
    error_hbm,
    warm_hbm,
    new_nodes_hbm,
    update_ref,
    new_error_ref,
    new_q_ref,
    node,
    edge,
    senders,
    receivers,
    send_index,
    cot,
    w_edge,
    w_node,
    error,
    warm,
    load_sem,
    store_sem,
    halo_out,
    halo_in,
    own_p,
    own_r,
    halo_p,
    pre,
    pick_halo,
    incidence,
    total,
    node_top,
    new_block,
    delta,
    inputs_t,
    grad_a,
    grad_b,
    ax_in,
    ax_sum,
    az_in,
    bz_in,
    b_sum,
    bx_in,
    matrix,
    dp_out,
    dp_in,
    z_out,
    z_in,
    x_out,
    x_in,
    q_out,
    q_in,
    gram_half,
    gram_out,
    gram_in,
    halo_s,
    halo_r,
    ax_s,
    ax_r,
    az_s,
    az_r,
    bz_s,
    bz_r,
    bx_s,
    bx_r,
    dp_s,
    dp_r,
    z_s,
    z_r,
    x_s,
    x_r,
    q_s,
    q_r,
    gram_s,
    gram_r,
):
    nz, nx, ny, nc, cut, tile = sizes
    ng, nd = nz * nx, ny * nc
    count, width = node.shape
    edges = edge.shape[0]
    tiles = edges // tile
    chunks = tile // LANE
    z, x = lax.axis_index(AXES[0]), lax.axis_index(AXES[1])
    y, c = lax.axis_index(AXES[2]), lax.axis_index(AXES[3])
    part = z * nx + x
    group = y * nc + c

    def on_graph(index):
        return (index // nx, lax.rem(index, nx), y, c)

    def on_dp(index):
        return (z, x, index // nc, lax.rem(index, nc))

    def on_z(index):
        return (index, x, y, c)

    def on_x(index):
        return (z, index, y, c)

    def remote(src, dst, send, recv, device):
        return pltpu.make_async_remote_copy(
            src_ref=src,
            dst_ref=dst,
            send_sem=send,
            recv_sem=recv,
            device_id=device,
            device_id_type=MESH,
        )

    loads = [
        pltpu.make_async_copy(src, dst, load_sem.at[i])
        for i, (src, dst) in enumerate(
            [
                (send_hbm, send_index),
                (node_hbm, node),
                (receivers_hbm, receivers),
                (senders_hbm, senders),
                (w_edge_hbm, w_edge),
                (edge_hbm, edge),
                (w_node_hbm, w_node),
                (cot_hbm, cot),
                (error_hbm, error),
                (warm_hbm, warm),
            ]
        )
    ]
    for load in loads:
        load.start()

    barrier = pltpu.get_barrier_semaphore()

    @pl.loop(1, ng)
    def _(o):
        pl.semaphore_signal(
            barrier, inc=1, device_id=on_graph(lax.rem(part + o, ng)), device_id_type=MESH
        )

    @pl.loop(1, nd)
    def _(o):
        pl.semaphore_signal(
            barrier, inc=1, device_id=on_dp(lax.rem(group + o, nd)), device_id_type=MESH
        )

    loads[0].wait()
    loads[1].wait()
    half = width // 2
    peer = send_index.shape[0] * LANE // ng
    per = LANE // peer
    for i in range(send_index.shape[0]):
        col = column(send_index[i : i + 1, :].astype(F32))
        rows = mm(one_hot(col, count), node[...])
        pair = jnp.concatenate(
            [
                rows[:, :half].reshape(per, peer, half),
                rows[:, half:].reshape(per, peer, half),
            ],
            axis=1,
        )
        halo_out[i * per : (i + 1) * per] = pair.astype(BF)
    halo_in[pl.ds(part, 1)] = halo_out[pl.ds(part, 1)]

    pl.semaphore_wait(barrier, ng - 1 + nd - 1)

    z_order = sorted(range(1, nz), key=lambda o: -min(o, nz - o))
    x_order = sorted(range(1, nx), key=lambda o: -min(o, nx - o))
    y_order = sorted(range(1, ny), key=lambda o: -min(o, ny - o))

    def z_at(o):
        return lax.rem(z + o, nz)

    def x_at(o):
        return lax.rem(x + o, nx)

    def halo_copy(i, oz, ox):
        to = z_at(oz) * nx + x_at(ox)
        return remote(
            halo_out.at[to],
            halo_in.at[part],
            halo_s.at[i],
            halo_r.at[i],
            (z_at(oz), x_at(ox), y, c),
        )

    halo_steps = [(oz, ox) for oz in z_order + [0] for ox in x_order + [0] if oz or ox]
    halo_copies = [halo_copy(i, *step) for i, step in enumerate(halo_steps)]
    for copy in halo_copies:
        copy.start()

    loads[2].wait()
    loads[3].wait()
    loads[4].wait()
    own_p[...] = mm(node[...], w_edge[width : 2 * width, :]).astype(BF)
    own_r[...] = mm(node[...], w_edge[2 * width :, :]).astype(BF)
    loads[5].wait()

    @pl.loop(0, tiles)
    def _(t):
        at = pl.ds(pl.multiple_of(t * tile, tile), tile)
        from_col = jnp.concatenate(
            [
                column(senders[pl.ds(t * chunks + j, 1), :].astype(F32))
                for j in range(chunks)
            ],
            axis=0,
        )
        to_rows = [receivers[pl.ds(t * chunks + j, 1), :].astype(F32) for j in range(chunks)]
        to_col = jnp.concatenate([column(row) for row in to_rows], axis=0)
        value = mm(edge[at, :], w_edge[:width, :])
        value = value + mm(one_hot(from_col, count), own_p[...])
        value = value + mm(one_hot(to_col, count), own_r[...])
        pre[at, :] = value
        pick_halo[at, :] = one_hot(from_col, halo_p.shape[0], count)
        ids = lax.broadcasted_iota(jnp.int32, (count, LANE), 0).astype(F32)
        for j, row in enumerate(to_rows):
            incidence[t, :, j * LANE : (j + 1) * LANE] = jnp.where(ids == row, 1.0, 0.0).astype(BF)

    inputs_t[:width, :] = node[...].astype(F32).T.astype(BF)

    loads[6].wait()
    node_top[...] = mm(node[...], w_node[:width, :])
    for copy in halo_copies:
        copy.wait()

    flat = halo_in[...].reshape(ng * 2 * peer, half)
    left_half = mm(flat, w_edge[width : width + half, :]).reshape(ng, 2, peer, width)
    right_half = mm(flat, w_edge[width + half : 2 * width, :]).reshape(ng, 2, peer, width)
    halo_p[...] = (left_half[:, 0] + right_half[:, 1]).reshape(ng * peer, width).astype(BF)

    total[...] = jnp.zeros_like(total)

    @pl.loop(0, tiles)
    def _(t):
        at = pl.ds(pl.multiple_of(t * tile, tile), tile)
        value = pre[at, :] + mm(pick_halo[at, :], halo_p[...])
        fresh = (edge[at, :].astype(F32) + value * sigmoid(value)).astype(BF)
        total[...] += mm(incidence[t], fresh)

    loads[7].wait()
    summed = total[...].astype(BF)
    node_pre = node_top[...] + mm(summed, w_node[width:, :])
    gate = sigmoid(node_pre)
    delta[...] = (cot[...].astype(F32) * (gate * (1.0 + node_pre * (1.0 - gate)))).astype(BF)
    new_block[...] = (node[...].astype(F32) + node_pre * gate).astype(BF)
    store = pltpu.make_async_copy(new_block, new_nodes_hbm, store_sem.at[0])
    store.start()
    inputs_t[width:, :] = total[...].T.astype(BF)

    share = 2 * width // ng
    turns = z_order + [0]
    bz = {
        o: remote(
            grad_b.at[z_at(o)], bz_in.at[o - 1], bz_s.at[o - 1], bz_r.at[o - 1], on_z(z_at(o))
        )
        for o in z_order
    }
    ax = {
        (t, o): remote(
            grad_a.at[z_at(t), x_at(o)],
            ax_in.at[o - 1, t],
            ax_s.at[o - 1, t],
            ax_r.at[o - 1, t],
            on_x(x_at(o)),
        )
        for t in turns
        for o in x_order
    }
    az = {
        o: remote(ax_sum.at[o], az_in.at[o - 1], az_s.at[o - 1], az_r.at[o - 1], on_z(z_at(o)))
        for o in z_order
    }
    bx = {
        o: remote(
            b_sum.at[x_at(o)], bx_in.at[o - 1], bx_s.at[o - 1], bx_r.at[o - 1], on_x(x_at(o))
        )
        for o in x_order
    }
    lines = nx * share
    for t in turns:
        at = pl.ds(pl.multiple_of(z_at(t) * lines, lines), lines)
        grad = mm(inputs_t[at, :], delta[...])
        grad_a[z_at(t)] = grad[:, :cut].reshape(nx, share, cut).astype(BF)
        grad_b[z_at(t)] = grad[:, cut:].reshape(nx, share, width - cut).astype(BF)
        for o in x_order:
            ax[t, o].start()
        if t:
            bz[t].start()
    for t in turns:
        value = grad_a[z_at(t), x].astype(F32)
        for o in x_order:
            ax[t, o].wait_recv()
            value = value + ax_in[o - 1, t].astype(F32)
        if t:
            ax_sum[t] = value.astype(BF)
            az[t].start()
        else:
            own_a = value
    value = grad_b[z].astype(F32)
    for o in z_order:
        bz[o].wait_recv()
        value = value + bz_in[o - 1].astype(F32)
    b_sum[...] = value.astype(BF)
    for copy in bx.values():
        copy.start()
    own_b = b_sum[x].astype(F32)
    for o in x_order:
        bx[o].wait_recv()
        own_b = own_b + bx_in[o - 1].astype(F32)
    for o in z_order:
        az[o].wait_recv()
        own_a = own_a + az_in[o - 1].astype(F32)
    loads[8].wait()
    loads[9].wait()
    matrix[:, :cut] = own_a + error[:, :cut]
    matrix[:, cut:] = own_b + error[:, cut:]

    rank = warm.shape[0]
    pack = LANE // rank
    blocks = width // LANE
    piece = LANE // nd
    local = mm(matrix[...], warm[...], ((1,), (1,)), HIGH)
    packed = jnp.concatenate([local[: share // 2], local[share // 2 :]], axis=1)
    turned = jnp.concatenate(
        [matrix[:, q * LANE : (q + 1) * LANE] for q in range(blocks)], axis=0
    ).T
    dp_out[:, :piece, :] = turned.reshape(nd, piece, LANE)
    dp_out[:, piece:, :] = jnp.broadcast_to(packed[None], (nd, *packed.shape))
    dp_in[pl.ds(group, 1)] = dp_out[pl.ds(group, 1)]

    dp_steps = [(oy, oc) for oy in y_order + [0] for oc in range(nc) if oy or oc]

    def dp_at(oy, oc):
        return (z, x, lax.rem(y + oy, ny), lax.rem(c + oc, nc))

    def member(device):
        return device[2] * nc + device[3]

    dp_copies = []
    for i, step in enumerate(dp_steps):
        to = dp_at(*step)
        dp_copies.append(
            remote(dp_out.at[member(to)], dp_in.at[group], dp_s.at[i], dp_r.at[i], to)
        )
    for copy in dp_copies:
        copy.start()
    for copy in dp_copies:
        copy.wait()

    arrived = jnp.sum(dp_in[...], axis=0)
    columns, packed = arrived[:piece], arrived[piece:]
    left = jnp.concatenate([packed[:, :rank], packed[:, rank:]], axis=0)
    gram = mm(left, left, ((0,), (0,)), HIGH)
    twice = jnp.concatenate([left, left], axis=1)
    spread = jnp.concatenate([twice] * blocks, axis=0)
    owner = lax.broadcasted_iota(jnp.int32, (LANE, LANE), 0) // share
    side = lax.broadcasted_iota(jnp.int32, (LANE, LANE), 1) // rank
    halves = blocks // pack
    for h in range(halves):
        chosen = jnp.where(owner == pack * h + side, spread, 0.0)
        z_out[h * piece : (h + 1) * piece, :] = mm(columns, chosen, precision=HIGH)
    both_parts = jnp.concatenate([gram[: rank // 2], gram[rank // 2 :]], axis=1)
    gram_half[...] = both_parts.reshape(nc, rank // 2 // nc, LANE)
    z_out[halves * piece :, :] = gram_half[c]

    z_in[pl.ds(z, 1)] = z_out[...][None]
    zs = {
        o: remote(z_out, z_in.at[z], z_s.at[o - 1], z_r.at[o - 1], on_z(z_at(o)))
        for o in z_order
    }
    for copy in zs.values():
        copy.start()
    for copy in zs.values():
        copy.wait()
    x_out[...] = jnp.sum(z_in[...], axis=0)
    x_in[pl.ds(x, 1)] = x_out[...][None]
    xs = {
        o: remote(x_out, x_in.at[x], x_s.at[o - 1], x_r.at[o - 1], on_x(x_at(o)))
        for o in x_order
    }
    for copy in xs.values():
        copy.start()
    for copy in xs.values():
        copy.wait()
    both = jnp.sum(x_in[...], axis=0)

    q_out[...] = both[: halves * piece]
    q_in[pl.ds(group, 1)] = q_out[...][None]

    q_copies = [
        remote(q_out, q_in.at[group], q_s.at[i], q_r.at[i], dp_at(*step))
        for i, step in enumerate(dp_steps)
    ]
    swap = remote(
        gram_out, gram_in.at[c], gram_s.at[0], gram_r.at[0], (z, x, y, lax.rem(c + 1, nc))
    )
    gram_out[...] = both[halves * piece :]
    gram_in[pl.ds(c, 1)] = gram_out[...][None]
    swap.start()
    for copy in q_copies:
        copy.start()
    swap.wait()
    packed = gram_in[...].reshape(rank // 2, LANE)
    gram = jnp.concatenate([packed[:, :rank], packed[:, rank:]], axis=0)
    inverse = inverse_factor(gram)
    ortho = mm(left, inverse, ((1,), (1,)), HIGH)

    for copy in q_copies:
        copy.wait()

    for h in range(halves):
        right = q_in[:, h * piece : (h + 1) * piece, :].reshape(LANE, LANE)
        for side in range(pack):
            q = h * pack + side
            at = slice(q * LANE, (q + 1) * LANE)
            new_q = mm(inverse, right[:, side * rank : (side + 1) * rank], ((1,), (1,)), HIGH) / nd
            new_q_ref[:, at] = new_q
            update = mm(ortho, new_q, precision=HIGH)
            update_ref[:, at] = update
            new_error_ref[:, at] = matrix[:, at] - update

    for copies in (bz, ax, az, bx):
        for copy in copies.values():
            copy.wait_send()
    store.wait()


def put(count, *refs):
    sources, results, sem = refs[:count], refs[count:-1], refs[-1]
    copies = [
        pltpu.make_async_copy(source, result, sem.at[i])
        for i, (source, result) in enumerate(zip(sources, results))
    ]
    for copy in copies:
        copy.start()
    for copy in copies:
        copy.wait()


def settled(*arrays):
    count = len(arrays)
    return pl.pallas_call(
        functools.partial(put, count),
        out_shape=tuple(jax.ShapeDtypeStruct(a.shape, a.dtype) for a in arrays),
        in_specs=[pl.BlockSpec(memory_space=pltpu.VMEM)] * count,
        out_specs=tuple([pl.BlockSpec(memory_space=pltpu.MemorySpace.HBM)] * count),
        scratch_shapes=[pltpu.SemaphoreType.DMA((count,))],
        compiler_params=pltpu.CompilerParams(vmem_limit_bytes=67043328),
    )(*arrays)


def layer(
    sizes,
    node_state,
    edge_state,
    senders,
    receivers,
    send_index,
    cotangent,
    w_edge,
    w_node,
    error_memory,
    warm_q,
):
    nz, nx, ny, nc, cut, tile = sizes
    ng, nd = nz * nx, ny * nc
    count, width = node_state.shape[1:]
    edges = edge_state.shape[1]
    rank = warm_q.shape[1]
    share = 2 * width // ng
    halo = send_index.shape[-1]
    peer = halo // ng
    piece = LANE // nd
    halves = width * rank // LANE // LANE
    hbm = pl.BlockSpec(memory_space=pltpu.MemorySpace.HBM)
    vmem = pl.BlockSpec(memory_space=pltpu.VMEM)
    dma = pltpu.SemaphoreType.DMA
    exchange = halves * piece + rank // 2 // nc
    new_block, update, new_error, new_q = pl.pallas_call(
        functools.partial(kernel, sizes),
        out_shape=(
            jax.ShapeDtypeStruct((count, width), BF),
            jax.ShapeDtypeStruct((share, width), F32),
            jax.ShapeDtypeStruct((share, width), F32),
            jax.ShapeDtypeStruct((rank, width), F32),
        ),
        in_specs=[hbm] * 10,
        out_specs=(hbm, vmem, vmem, vmem),
        scratch_shapes=[
            pltpu.VMEM((count, width), BF),
            pltpu.VMEM((edges, width), BF),
            pltpu.VMEM((edges // LANE, LANE), jnp.int32),
            pltpu.VMEM((edges // LANE, LANE), jnp.int32),
            pltpu.VMEM((halo // LANE, LANE), jnp.int32),
            pltpu.VMEM((count, width), BF),
            pltpu.VMEM((3 * width, width), BF),
            pltpu.VMEM((2 * width, width), BF),
            pltpu.VMEM((share, width), F32),
            pltpu.VMEM((rank, width), F32),
            dma((10,)),
            dma((1,)),
            pltpu.VMEM((ng, 2 * peer, width // 2), BF),
            pltpu.VMEM((ng, 2 * peer, width // 2), BF),
            pltpu.VMEM((count, width), BF),
            pltpu.VMEM((count, width), BF),
            pltpu.VMEM((halo, width), BF),
            pltpu.VMEM((edges, width), F32),
            pltpu.VMEM((edges, halo), BF),
            pltpu.VMEM((edges // tile, count, tile), BF),
            pltpu.VMEM((count, width), F32),
            pltpu.VMEM((count, width), F32),
            pltpu.VMEM((count, width), BF),
            pltpu.VMEM((count, width), BF),
            pltpu.VMEM((2 * width, count), BF),
            pltpu.VMEM((nz, nx, share, cut), BF),
            pltpu.VMEM((nz, nx, share, width - cut), BF),
            pltpu.VMEM((nx - 1, nz, share, cut), BF),
            pltpu.VMEM((nz, share, cut), BF),
            pltpu.VMEM((nz - 1, share, cut), BF),
            pltpu.VMEM((nz - 1, nx, share, width - cut), BF),
            pltpu.VMEM((nx, share, width - cut), BF),
            pltpu.VMEM((nx - 1, share, width - cut), BF),
            pltpu.VMEM((share, width), F32),
            pltpu.VMEM((nd, piece + share // 2, LANE), F32),
            pltpu.VMEM((nd, piece + share // 2, LANE), F32),
            pltpu.VMEM((exchange, LANE), F32),
            pltpu.VMEM((nz, exchange, LANE), F32),
            pltpu.VMEM((exchange, LANE), F32),
            pltpu.VMEM((nx, exchange, LANE), F32),
            pltpu.VMEM((halves * piece, LANE), F32),
            pltpu.VMEM((nd, halves * piece, LANE), F32),
            pltpu.VMEM((nc, rank // 2 // nc, LANE), F32),
            pltpu.VMEM((rank // 2 // nc, LANE), F32),
            pltpu.VMEM((nc, rank // 2 // nc, LANE), F32),
            dma((ng - 1,)),
            dma((ng - 1,)),
            dma((nx - 1, nz)),
            dma((nx - 1, nz)),
            dma((nz - 1,)),
            dma((nz - 1,)),
            dma((nz - 1,)),
            dma((nz - 1,)),
            dma((nx - 1,)),
            dma((nx - 1,)),
            dma((nd - 1,)),
            dma((nd - 1,)),
            dma((nz - 1,)),
            dma((nz - 1,)),
            dma((nx - 1,)),
            dma((nx - 1,)),
            dma((nd - 1,)),
            dma((nd - 1,)),
            dma((1,)),
            dma((1,)),
        ],
        compiler_params=pltpu.CompilerParams(
            collective_id=0, has_side_effects=True, vmem_limit_bytes=67043328
        ),
    )(
        node_state[0],
        edge_state[0],
        senders.reshape(-1, LANE),
        receivers.reshape(-1, LANE),
        send_index.reshape(-1, LANE),
        cotangent[0],
        w_edge,
        w_node,
        error_memory[0],
        warm_q.T,
    )
    new_block, update, new_error, new_q = settled(new_block, update, new_error, new_q)
    return new_block[None], update, new_error[None], new_q.T


def build(finer, cut, tile):
    placed = (
        P(DP, GRAPH, None),
        P(DP, GRAPH, None),
        P(DP, GRAPH),
        P(DP, GRAPH),
        P(DP, GRAPH, None),
        P(DP, GRAPH, None),
        P(),
        P(),
        P(DP, GRAPH, None),
        P(),
    )
    sizes = (*(finer.shape[a] for a in AXES), cut, tile)
    return jax.shard_map(
        functools.partial(layer, sizes),
        mesh=finer,
        in_specs=placed,
        out_specs=(P(DP, GRAPH, None), P(GRAPH, None), P(DP, GRAPH, None), P()),
        check_vma=False,
    )


def solution(mesh):
    return build(Mesh(mesh.devices.reshape(8, 4, 8, 2), AXES), 384, 512)
```

```python
import functools

import jax
import jax.numpy as jnp
from jax import lax
from jax.experimental import pallas as pl
from jax.experimental.pallas import tpu as pltpu
from jax.sharding import Mesh
from jax.sharding import PartitionSpec as P

AXES = ("graph_0", "graph_1", "dp_0", "dp_1")
GRAPH = AXES[:2]
DP = AXES[2:]
MESH = pl.DeviceIdType.MESH
BF = jnp.bfloat16
F32 = jnp.float32
HIGH = lax.Precision.HIGHEST
LANE = 128


def mm(a, b, dims=((1,), (0,)), precision=None):
    return lax.dot_general(a, b, (dims, ((), ())), precision=precision, preferred_element_type=F32)


def sigmoid(v):
    return 0.5 + 0.5 * jnp.tanh(0.5 * v)


def column(row):
    eye = lax.broadcasted_iota(jnp.int32, (LANE, LANE), 0) == lax.broadcasted_iota(
        jnp.int32, (LANE, LANE), 1
    )
    return jnp.sum(jnp.where(eye, row, 0.0), axis=1, keepdims=True)


def one_hot(col, width, base=0):
    lanes = lax.broadcasted_iota(jnp.int32, (col.shape[0], width), 1) + base
    return jnp.where(lanes.astype(F32) == col, 1.0, 0.0).astype(BF)


def inverse_factor(gram):
    n = gram.shape[0]
    rows = lax.broadcasted_iota(jnp.int32, (n, 1), 0)
    eye = jnp.where(
        lax.broadcasted_iota(jnp.int32, (n, n), 0) == lax.broadcasted_iota(jnp.int32, (n, n), 1),
        1.0,
        0.0,
    ).astype(F32)
    work = jnp.concatenate([gram, eye], axis=1)
    for k in range(n - 1):
        pivot = work[k : k + 1, :]
        scaled = pivot / pivot[:, k : k + 1]
        work = work - jnp.where(rows > k, work[:, k : k + 1], 0.0) * scaled
    diagonal = jnp.sum(work[:, :n] * eye, axis=1, keepdims=True)
    return work[:, n:] / jnp.sqrt(diagonal)


def kernel(
    sizes,
    node_hbm,
    edge_hbm,
    senders_hbm,
    receivers_hbm,
    send_hbm,
    cot_hbm,
    w_edge_hbm,
    w_node_hbm,
    error_hbm,
    warm_hbm,
    new_nodes_hbm,
    update_ref,
    new_error_ref,
    new_q_ref,
    node,
    edge,
    senders,
    receivers,
    send_index,
    cot,
    w_edge,
    w_node,
    error,
    warm,
    load_sem,
    store_sem,
    halo_out,
    halo_in,
    own_p,
    own_r,
    halo_p,
    pre,
    pick_halo,
    incidence,
    total,
    node_top,
    new_block,
    delta,
    inputs_t,
    grad_a,
    grad_b,
    ax_in,
    ax_sum,
    az_in,
    bz_in,
    b_sum,
    bx_in,
    matrix,
    dp_out,
    dp_in,
    z_out,
    z_in,
    x_out,
    x_in,
    q_out,
    q_in,
    gram_half,
    zg_out,
    zg_in,
    xg_out,
    xg_in,
    gram_out,
    gram_in,
    halo_s,
    halo_r,
    ax_s,
    ax_r,
    az_s,
    az_r,
    bz_s,
    bz_r,
    bx_s,
    bx_r,
    dp_s,
    dp_r,
    z_s,
    z_r,
    x_s,
    x_r,
    q_s,
    q_r,
    gram_s,
    gram_r,
    zg_s,
    zg_r,
    xg_s,
    xg_r,
):
    nz, nx, ny, nc, cut, tile = sizes
    ng, nd = nz * nx, ny * nc
    count, width = node.shape
    edges = edge.shape[0]
    tiles = edges // tile
    chunks = tile // LANE
    z, x = lax.axis_index(AXES[0]), lax.axis_index(AXES[1])
    y, c = lax.axis_index(AXES[2]), lax.axis_index(AXES[3])
    part = z * nx + x
    group = y * nc + c

    def on_graph(index):
        return (index // nx, lax.rem(index, nx), y, c)

    def on_dp(index):
        return (z, x, index // nc, lax.rem(index, nc))

    def on_z(index):
        return (index, x, y, c)

    def on_x(index):
        return (z, index, y, c)

    def remote(src, dst, send, recv, device):
        return pltpu.make_async_remote_copy(
            src_ref=src,
            dst_ref=dst,
            send_sem=send,
            recv_sem=recv,
            device_id=device,
            device_id_type=MESH,
        )

    loads = [
        pltpu.make_async_copy(src, dst, load_sem.at[i])
        for i, (src, dst) in enumerate(
            [
                (send_hbm, send_index),
                (node_hbm, node),
                (receivers_hbm, receivers),
                (senders_hbm, senders),
                (w_edge_hbm, w_edge),
                (edge_hbm, edge),
                (w_node_hbm, w_node),
                (cot_hbm, cot),
                (error_hbm, error),
                (warm_hbm, warm),
            ]
        )
    ]
    for load in loads:
        load.start()

    barrier = pltpu.get_barrier_semaphore()

    @pl.loop(1, ng)
    def _(o):
        pl.semaphore_signal(
            barrier, inc=1, device_id=on_graph(lax.rem(part + o, ng)), device_id_type=MESH
        )

    @pl.loop(1, nd)
    def _(o):
        pl.semaphore_signal(
            barrier, inc=1, device_id=on_dp(lax.rem(group + o, nd)), device_id_type=MESH
        )

    loads[0].wait()
    loads[1].wait()
    half = width // 2
    peer = send_index.shape[0] * LANE // ng
    per = LANE // peer
    for i in range(send_index.shape[0]):
        col = column(send_index[i : i + 1, :].astype(F32))
        rows = mm(one_hot(col, count), node[...])
        pair = jnp.concatenate(
            [
                rows[:, :half].reshape(per, peer, half),
                rows[:, half:].reshape(per, peer, half),
            ],
            axis=1,
        )
        halo_out[i * per : (i + 1) * per] = pair.astype(BF)
    halo_in[pl.ds(part, 1)] = halo_out[pl.ds(part, 1)]

    pl.semaphore_wait(barrier, ng - 1 + nd - 1)

    z_order = sorted(range(1, nz), key=lambda o: -min(o, nz - o))
    x_order = sorted(range(1, nx), key=lambda o: -min(o, nx - o))
    y_order = sorted(range(1, ny), key=lambda o: -min(o, ny - o))
    z_near = sorted(range(1, nz), key=lambda o: min(o, nz - o))

    def z_at(o):
        return lax.rem(z + o, nz)

    def x_at(o):
        return lax.rem(x + o, nx)

    def halo_copy(i, oz, ox):
        to = z_at(oz) * nx + x_at(ox)
        return remote(
            halo_out.at[to],
            halo_in.at[part],
            halo_s.at[i],
            halo_r.at[i],
            (z_at(oz), x_at(ox), y, c),
        )

    halo_steps = [(oz, ox) for ox in range(nx) for oz in z_near + [0] if oz or ox]
    halo_copies = [halo_copy(i, *step) for i, step in enumerate(halo_steps)]
    for copy in halo_copies:
        copy.start()

    loads[2].wait()
    loads[3].wait()
    loads[4].wait()
    own_p[...] = mm(node[...], w_edge[width : 2 * width, :]).astype(BF)
    own_r[...] = mm(node[...], w_edge[2 * width :, :]).astype(BF)
    loads[5].wait()

    @pl.loop(0, tiles)
    def _(t):
        at = pl.ds(pl.multiple_of(t * tile, tile), tile)
        from_col = jnp.concatenate(
            [
                column(senders[pl.ds(t * chunks + j, 1), :].astype(F32))
                for j in range(chunks)
            ],
            axis=0,
        )
        to_rows = [receivers[pl.ds(t * chunks + j, 1), :].astype(F32) for j in range(chunks)]
        to_col = jnp.concatenate([column(row) for row in to_rows], axis=0)
        value = mm(edge[at, :], w_edge[:width, :])
        value = value + mm(one_hot(from_col, count), own_p[...])
        value = value + mm(one_hot(to_col, count), own_r[...])
        pre[at, :] = value
        pick_halo[at, :] = one_hot(from_col, halo_p.shape[0], count)
        ids = lax.broadcasted_iota(jnp.int32, (count, LANE), 0).astype(F32)
        for j, row in enumerate(to_rows):
            incidence[t, :, j * LANE : (j + 1) * LANE] = jnp.where(ids == row, 1.0, 0.0).astype(BF)

    inputs_t[:width, :] = node[...].astype(F32).T.astype(BF)

    loads[6].wait()
    node_top[...] = mm(node[...], w_node[:width, :])
    for copy in halo_copies:
        copy.wait()

    flat = halo_in[...].reshape(ng * 2 * peer, half)
    left_half = mm(flat, w_edge[width : width + half, :]).reshape(ng, 2, peer, width)
    right_half = mm(flat, w_edge[width + half : 2 * width, :]).reshape(ng, 2, peer, width)
    halo_p[...] = (left_half[:, 0] + right_half[:, 1]).reshape(ng * peer, width).astype(BF)

    total[...] = jnp.zeros_like(total)

    @pl.loop(0, tiles)
    def _(t):
        at = pl.ds(pl.multiple_of(t * tile, tile), tile)
        value = pre[at, :] + mm(pick_halo[at, :], halo_p[...])
        fresh = (edge[at, :].astype(F32) + value * sigmoid(value)).astype(BF)
        total[...] += mm(incidence[t], fresh)

    loads[7].wait()
    summed = total[...].astype(BF)
    node_pre = node_top[...] + mm(summed, w_node[width:, :])
    gate = sigmoid(node_pre)
    delta[...] = (cot[...].astype(F32) * (gate * (1.0 + node_pre * (1.0 - gate)))).astype(BF)
    new_block[...] = (node[...].astype(F32) + node_pre * gate).astype(BF)
    store = pltpu.make_async_copy(new_block, new_nodes_hbm, store_sem.at[0])
    store.start()
    inputs_t[width:, :] = total[...].T.astype(BF)

    share = 2 * width // ng
    turns = z_order + [0]
    bz = {
        o: remote(
            grad_b.at[z_at(o)], bz_in.at[o - 1], bz_s.at[o - 1], bz_r.at[o - 1], on_z(z_at(o))
        )
        for o in z_order
    }
    ax = {
        (t, o): remote(
            grad_a.at[z_at(t), x_at(o)],
            ax_in.at[o - 1, t],
            ax_s.at[o - 1, t],
            ax_r.at[o - 1, t],
            on_x(x_at(o)),
        )
        for t in turns
        for o in x_order
    }
    az = {
        o: remote(ax_sum.at[o], az_in.at[o - 1], az_s.at[o - 1], az_r.at[o - 1], on_z(z_at(o)))
        for o in z_order
    }
    bx = {
        o: remote(
            b_sum.at[x_at(o)], bx_in.at[o - 1], bx_s.at[o - 1], bx_r.at[o - 1], on_x(x_at(o))
        )
        for o in x_order
    }
    lines = nx * share
    for t in turns:
        at = pl.ds(pl.multiple_of(z_at(t) * lines, lines), lines)
        grad = mm(inputs_t[at, :], delta[...])
        grad_a[z_at(t)] = grad[:, :cut].reshape(nx, share, cut).astype(BF)
        grad_b[z_at(t)] = grad[:, cut:].reshape(nx, share, width - cut).astype(BF)
        for o in x_order:
            ax[t, o].start()
        if t:
            bz[t].start()
    for t in turns:
        value = grad_a[z_at(t), x].astype(F32)
        for o in x_order:
            ax[t, o].wait_recv()
            value = value + ax_in[o - 1, t].astype(F32)
        if t:
            ax_sum[t] = value.astype(BF)
            az[t].start()
        else:
            own_a = value
    value = grad_b[z].astype(F32)
    for o in z_order:
        bz[o].wait_recv()
        value = value + bz_in[o - 1].astype(F32)
    b_sum[...] = value.astype(BF)
    for copy in bx.values():
        copy.start()
    own_b = b_sum[x].astype(F32)
    for o in x_order:
        bx[o].wait_recv()
        own_b = own_b + bx_in[o - 1].astype(F32)
    for o in z_order:
        az[o].wait_recv()
        own_a = own_a + az_in[o - 1].astype(F32)
    loads[8].wait()
    loads[9].wait()
    matrix[:, :cut] = own_a + error[:, :cut]
    matrix[:, cut:] = own_b + error[:, cut:]

    rank = warm.shape[0]
    pack = LANE // rank
    blocks = width // LANE
    piece = LANE // nd
    local = mm(matrix[...], warm[...], ((1,), (1,)), HIGH)
    packed = jnp.concatenate([local[: share // 2], local[share // 2 :]], axis=1)
    turned = jnp.concatenate(
        [matrix[:, q * LANE : (q + 1) * LANE] for q in range(blocks)], axis=0
    ).T
    dp_out[:, :piece, :] = turned.reshape(nd, piece, LANE)
    dp_out[:, piece:, :] = jnp.broadcast_to(packed[None], (nd, *packed.shape))
    dp_in[pl.ds(group, 1)] = dp_out[pl.ds(group, 1)]

    dp_steps = [(oy, oc) for oy in y_order + [0] for oc in range(nc) if oy or oc]

    def dp_at(oy, oc):
        return (z, x, lax.rem(y + oy, ny), lax.rem(c + oc, nc))

    def member(device):
        return device[2] * nc + device[3]

    dp_copies = []
    for i, step in enumerate(dp_steps):
        to = dp_at(*step)
        dp_copies.append(
            remote(dp_out.at[member(to)], dp_in.at[group], dp_s.at[i], dp_r.at[i], to)
        )
    for copy in dp_copies:
        copy.start()
    for copy in dp_copies:
        copy.wait()

    arrived = jnp.sum(dp_in[...], axis=0)
    columns, packed = arrived[:piece], arrived[piece:]
    left = jnp.concatenate([packed[:, :rank], packed[:, rank:]], axis=0)
    gram = mm(left, left, ((0,), (0,)), HIGH)
    twice = jnp.concatenate([left, left], axis=1)
    spread = jnp.concatenate([twice] * blocks, axis=0)
    owner = lax.broadcasted_iota(jnp.int32, (LANE, LANE), 0) // share
    side = lax.broadcasted_iota(jnp.int32, (LANE, LANE), 1) // rank
    halves = blocks // pack
    for h in range(halves):
        chosen = jnp.where(owner == pack * h + side, spread, 0.0)
        z_out[h * piece : (h + 1) * piece, :] = mm(columns, chosen, precision=HIGH)
    both_parts = jnp.concatenate([gram[: rank // 2], gram[rank // 2 :]], axis=1)
    gram_half[...] = both_parts.reshape(nc, rank // 2 // nc, LANE)
    zg_out[...] = gram_half[c]

    def to_all(order, out, into, me, send, recv, device):
        into[pl.ds(me, 1)] = out[...][None]
        return [
            remote(out, into.at[me], send.at[o - 1], recv.at[o - 1], device(o)) for o in order
        ]

    def along_z(o):
        return on_z(z_at(o))

    def along_x(o):
        return on_x(x_at(o))

    zg = to_all(z_order, zg_out, zg_in, z, zg_s, zg_r, along_z)
    for copy in zg:
        copy.start()
    zs = to_all(z_order, z_out, z_in, z, z_s, z_r, along_z)
    for copy in zs:
        copy.start()
    for copy in zg:
        copy.wait()
    xg_out[...] = jnp.sum(zg_in[...], axis=0)
    xg = to_all(x_order, xg_out, xg_in, x, xg_s, xg_r, along_x)
    for copy in xg:
        copy.start()
    for copy in zs:
        copy.wait()
    x_out[...] = jnp.sum(z_in[...], axis=0)
    xs = to_all(x_order, x_out, x_in, x, x_s, x_r, along_x)
    for copy in xs:
        copy.start()
    for copy in xg:
        copy.wait()
    gram_out[...] = jnp.sum(xg_in[...], axis=0)
    gram_in[pl.ds(c, 1)] = gram_out[...][None]
    swap = remote(
        gram_out, gram_in.at[c], gram_s.at[0], gram_r.at[0], (z, x, y, lax.rem(c + 1, nc))
    )
    swap.start()
    for copy in xs:
        copy.wait()

    q_out[...] = jnp.sum(x_in[...], axis=0)
    q_in[pl.ds(group, 1)] = q_out[...][None]

    q_copies = [
        remote(q_out, q_in.at[group], q_s.at[i], q_r.at[i], dp_at(*step))
        for i, step in enumerate(dp_steps)
    ]
    for copy in q_copies:
        copy.start()
    swap.wait()
    packed = gram_in[...].reshape(rank // 2, LANE)
    gram = jnp.concatenate([packed[:, :rank], packed[:, rank:]], axis=0)
    inverse = inverse_factor(gram)
    ortho = mm(left, inverse, ((1,), (1,)), HIGH)

    for copy in q_copies:
        copy.wait()

    for h in range(halves):
        right = q_in[:, h * piece : (h + 1) * piece, :].reshape(LANE, LANE)
        for side in range(pack):
            q = h * pack + side
            at = slice(q * LANE, (q + 1) * LANE)
            new_q = mm(inverse, right[:, side * rank : (side + 1) * rank], ((1,), (1,)), HIGH) / nd
            new_q_ref[:, at] = new_q
            update = mm(ortho, new_q, precision=HIGH)
            update_ref[:, at] = update
            new_error_ref[:, at] = matrix[:, at] - update

    for copies in (bz, ax, az, bx):
        for copy in copies.values():
            copy.wait_send()
    store.wait()


def put(count, *refs):
    sources, results, sem = refs[:count], refs[count:-1], refs[-1]
    copies = [
        pltpu.make_async_copy(source, result, sem.at[i])
        for i, (source, result) in enumerate(zip(sources, results))
    ]
    for copy in copies:
        copy.start()
    for copy in copies:
        copy.wait()


def settled(*arrays):
    count = len(arrays)
    return pl.pallas_call(
        functools.partial(put, count),
        out_shape=tuple(jax.ShapeDtypeStruct(a.shape, a.dtype) for a in arrays),
        in_specs=[pl.BlockSpec(memory_space=pltpu.VMEM)] * count,
        out_specs=tuple([pl.BlockSpec(memory_space=pltpu.MemorySpace.HBM)] * count),
        scratch_shapes=[pltpu.SemaphoreType.DMA((count,))],
        compiler_params=pltpu.CompilerParams(vmem_limit_bytes=67043328),
    )(*arrays)


def layer(
    sizes,
    node_state,
    edge_state,
    senders,
    receivers,
    send_index,
    cotangent,
    w_edge,
    w_node,
    error_memory,
    warm_q,
):
    nz, nx, ny, nc, cut, tile = sizes
    ng, nd = nz * nx, ny * nc
    count, width = node_state.shape[1:]
    edges = edge_state.shape[1]
    rank = warm_q.shape[1]
    share = 2 * width // ng
    halo = send_index.shape[-1]
    peer = halo // ng
    piece = LANE // nd
    halves = width * rank // LANE // LANE
    hbm = pl.BlockSpec(memory_space=pltpu.MemorySpace.HBM)
    vmem = pl.BlockSpec(memory_space=pltpu.VMEM)
    dma = pltpu.SemaphoreType.DMA
    exchange = halves * piece
    gram_rows = rank // 2 // nc
    new_block, update, new_error, new_q = pl.pallas_call(
        functools.partial(kernel, sizes),
        out_shape=(
            jax.ShapeDtypeStruct((count, width), BF),
            jax.ShapeDtypeStruct((share, width), F32),
            jax.ShapeDtypeStruct((share, width), F32),
            jax.ShapeDtypeStruct((rank, width), F32),
        ),
        in_specs=[hbm] * 10,
        out_specs=(hbm, vmem, vmem, vmem),
        scratch_shapes=[
            pltpu.VMEM((count, width), BF),
            pltpu.VMEM((edges, width), BF),
            pltpu.VMEM((edges // LANE, LANE), jnp.int32),
            pltpu.VMEM((edges // LANE, LANE), jnp.int32),
            pltpu.VMEM((halo // LANE, LANE), jnp.int32),
            pltpu.VMEM((count, width), BF),
            pltpu.VMEM((3 * width, width), BF),
            pltpu.VMEM((2 * width, width), BF),
            pltpu.VMEM((share, width), F32),
            pltpu.VMEM((rank, width), F32),
            dma((10,)),
            dma((1,)),
            pltpu.VMEM((ng, 2 * peer, width // 2), BF),
            pltpu.VMEM((ng, 2 * peer, width // 2), BF),
            pltpu.VMEM((count, width), BF),
            pltpu.VMEM((count, width), BF),
            pltpu.VMEM((halo, width), BF),
            pltpu.VMEM((edges, width), F32),
            pltpu.VMEM((edges, halo), BF),
            pltpu.VMEM((edges // tile, count, tile), BF),
            pltpu.VMEM((count, width), F32),
            pltpu.VMEM((count, width), F32),
            pltpu.VMEM((count, width), BF),
            pltpu.VMEM((count, width), BF),
            pltpu.VMEM((2 * width, count), BF),
            pltpu.VMEM((nz, nx, share, cut), BF),
            pltpu.VMEM((nz, nx, share, width - cut), BF),
            pltpu.VMEM((nx - 1, nz, share, cut), BF),
            pltpu.VMEM((nz, share, cut), BF),
            pltpu.VMEM((nz - 1, share, cut), BF),
            pltpu.VMEM((nz - 1, nx, share, width - cut), BF),
            pltpu.VMEM((nx, share, width - cut), BF),
            pltpu.VMEM((nx - 1, share, width - cut), BF),
            pltpu.VMEM((share, width), F32),
            pltpu.VMEM((nd, piece + share // 2, LANE), F32),
            pltpu.VMEM((nd, piece + share // 2, LANE), F32),
            pltpu.VMEM((exchange, LANE), F32),
            pltpu.VMEM((nz, exchange, LANE), F32),
            pltpu.VMEM((exchange, LANE), F32),
            pltpu.VMEM((nx, exchange, LANE), F32),
            pltpu.VMEM((halves * piece, LANE), F32),
            pltpu.VMEM((nd, halves * piece, LANE), F32),
            pltpu.VMEM((nc, gram_rows, LANE), F32),
            pltpu.VMEM((gram_rows, LANE), F32),
            pltpu.VMEM((nz, gram_rows, LANE), F32),
            pltpu.VMEM((gram_rows, LANE), F32),
            pltpu.VMEM((nx, gram_rows, LANE), F32),
            pltpu.VMEM((gram_rows, LANE), F32),
            pltpu.VMEM((nc, gram_rows, LANE), F32),
            dma((ng - 1,)),
            dma((ng - 1,)),
            dma((nx - 1, nz)),
            dma((nx - 1, nz)),
            dma((nz - 1,)),
            dma((nz - 1,)),
            dma((nz - 1,)),
            dma((nz - 1,)),
            dma((nx - 1,)),
            dma((nx - 1,)),
            dma((nd - 1,)),
            dma((nd - 1,)),
            dma((nz - 1,)),
            dma((nz - 1,)),
            dma((nx - 1,)),
            dma((nx - 1,)),
            dma((nd - 1,)),
            dma((nd - 1,)),
            dma((1,)),
            dma((1,)),
            dma((nz - 1,)),
            dma((nz - 1,)),
            dma((nx - 1,)),
            dma((nx - 1,)),
        ],
        compiler_params=pltpu.CompilerParams(
            collective_id=0, has_side_effects=True, vmem_limit_bytes=67043328
        ),
    )(
        node_state[0],
        edge_state[0],
        senders.reshape(-1, LANE),
        receivers.reshape(-1, LANE),
        send_index.reshape(-1, LANE),
        cotangent[0],
        w_edge,
        w_node,
        error_memory[0],
        warm_q.T,
    )
    new_block, update, new_error, new_q = settled(new_block, update, new_error, new_q)
    return new_block[None], update, new_error[None], new_q.T


def build(finer, cut, tile):
    placed = (
        P(DP, GRAPH, None),
        P(DP, GRAPH, None),
        P(DP, GRAPH),
        P(DP, GRAPH),
        P(DP, GRAPH, None),
        P(DP, GRAPH, None),
        P(),
        P(),
        P(DP, GRAPH, None),
        P(),
    )
    sizes = (*(finer.shape[a] for a in AXES), cut, tile)
    return jax.shard_map(
        functools.partial(layer, sizes),
        mesh=finer,
        in_specs=placed,
        out_specs=(P(DP, GRAPH, None), P(GRAPH, None), P(DP, GRAPH, None), P()),
        check_vma=False,
    )


def solution(mesh):
    return build(Mesh(mesh.devices.reshape(8, 4, 8, 2), AXES), 384, 512)
```
